32 devices in a mesh: heads: 4 (over y, core), batch: 8 (over z, x).
Axes of the slice: x: 2, y: 2, z: 4, core: 2. Of those that a mesh axis runs over, the one named last changes fastest.
Arguments:
- queries: bfloat16 [64, 4096], P('batch', 'heads'), may hold values from -6 to 6
- keys_new: bfloat16 [64, 4096], P('batch', 'heads'), may hold values from -6 to 6
- values_new: bfloat16 [64, 4096], P('batch', 'heads'), may hold values from -6 to 6
- out_gate: bfloat16 [64, 4096], P('batch', 'heads'), may hold values from -6 to 6
- decay_logit: float32 [64, 32], P('batch', 'heads'), may hold values from -6 to 6
- beta_logit: float32 [64, 32], P('batch', 'heads'), may hold values from -6 to 6
- decay_rate: float32 [32], P('heads'), may hold values from 0.05 to 2
- state: float32 [64, 32, 128, 128], P('batch', 'heads'), may hold values from -0.6 to 0.6
- norm_gain: float32 [128], replicated, may hold values from 0.1 to 1.9
- out_proj: bfloat16 [4096, 4096], P('heads'), may hold values from -0.09375 to 0.09375
- residual: bfloat16 [64, 4096], P('batch'), may hold values from -40 to 40, as said below
- final_gain: float32 [4096], replicated, may hold values from 0.1 to 1.9
- value_weight: float32 [4096], replicated, may hold values from -0.09375 to 0.09375
- lm_head: bfloat16 [4096, 4096], P(None, ('heads', 'batch')), may hold values from -15 to 15
- sampled: int32 [64], replicated, may hold values from 0 to 4095
Outputs:
- logprob: float32 [64], P('batch')
- value: float32 [64], P('batch')
The draws below stay inside these ranges and needn't reach their ends.
Inputs may be any that keep to these rules, and one draw needn't show every extreme that they name: The residual stream's entries have scales that differ by row and by column (up to tenfold each), so neither rows nor columns share one magnitude.
All inputs are finite; a program needn't handle non-finite values.
Results may differ from the reference program's by a relative error of at most 0.0013.
Values may be sent and summed in bfloat16 or wider, within the bound.
A program may use at most 64 MiB of HBM per device.

```python
import math
import jax
import jax.numpy as jnp
from jax import lax

D = 4096
H = 32
DK = 128
DV = 128
BATCH = 64
VOCAB = 4096


def draw_residual(key, part):
    first, second, third = jax.random.split(jax.random.fold_in(key, 11), 3)
    base = jnp.clip(jax.random.normal(first, (BATCH, D), jnp.float32), -4.0, 4.0)
    row_scale = jnp.exp(jax.random.uniform(second, (BATCH, 1), jnp.float32) * jnp.log(10.0))
    col_scale = jnp.exp(jax.random.uniform(third, (1, D), jnp.float32) * jnp.log(10.0))
    return (base * row_scale * col_scale * 0.1).astype(jnp.bfloat16)


def draw_lm_head(key, part):
    first = jax.random.fold_in(jax.random.fold_in(key, 23), 0)
    base = jnp.clip(jax.random.normal(first, (D, VOCAB), jnp.float32), -4.0, 4.0) * (3.0 / jnp.sqrt(D * 1.0))
    return base.astype(jnp.bfloat16)


def place_ends(entries, rng, smallest, largest):
    place = [jax.random.randint(jax.random.fold_in(rng, axis), (), 0, length) for axis, length in enumerate(entries.shape)]
    widest = entries.shape.index(max(entries.shape))
    neighbour = place[:widest] + [(place[widest] + 1) % entries.shape[widest]] + place[widest + 1:]
    return entries.at[tuple(place)].set(smallest).at[tuple(neighbour)].set(largest)


def shard_levels(own_key, extent, shards, low, top_value):
    factor_of, own = 1.0, jax.random.fold_in(own_key, 6)
    for dim, parts in shards:
        draws = jnp.exp(jax.random.uniform(jax.random.fold_in(own, dim), (parts,), jnp.float32, low / len(shards), top_value / len(shards)))
        factor_of = factor_of * jnp.repeat(draws, extent[dim] // parts).reshape([-1 if axis == dim else 1 for axis in range(len(extent))])
    return factor_of


def normal_values(key, dims, spread, bound, shards=(), kind=jnp.bfloat16):
    factor_of = shard_levels(key, dims, shards, -0.22, 0.18) if shards else 1.0
    entries = jax.random.normal(key, dims, jnp.float32) * spread * factor_of
    return jnp.minimum(jnp.maximum(entries, -bound), bound).astype(kind)


def setup_inputs(seed: int = 0) -> dict:
    key_list = jax.random.split(jax.random.key(seed), 16)
    return {
        "queries": normal_values(key_list[0], (BATCH, H * DK), 1.0, 6.0, ((0, 8), (1, 4))),
        "keys_new": normal_values(key_list[1], (BATCH, H * DK), 1.0, 6.0, ((0, 8), (1, 4))),
        "values_new": normal_values(key_list[2], (BATCH, H * DV), 1.0, 6.0, ((0, 8), (1, 4))),
        "out_gate": normal_values(key_list[3], (BATCH, H * DV), 1.0, 6.0, ((0, 8), (1, 4))),
        "decay_logit": normal_values(key_list[4], (BATCH, H), 1.5, 6.0, ((0, 8), (1, 4)), jnp.float32),
        "beta_logit": normal_values(key_list[5], (BATCH, H), 1.5, 6.0, ((0, 8), (1, 4)), jnp.float32),
        "decay_rate": jnp.clip(jnp.exp(math.log(2.0) - 3.6888794 * jax.random.uniform(key_list[6], (H,), jnp.float32) ** shard_levels(key_list[6], (H,), ((0, 4),), -0.2, 0.2)), 0.05, 2.0),
        "state": normal_values(key_list[7], (BATCH, H, DK, DV), 0.1, 0.6, ((0, 8), (1, 4)), jnp.float32),
        "norm_gain": jnp.clip(1.0 + 0.18 * jax.random.normal(key_list[8], (DV,), jnp.float32), 0.1, 1.9),
        "out_proj": normal_values(key_list[9], (H * DV, D), (H * DV) ** -0.5, 0.09375, ((0, 4),)),
        "residual": draw_residual(jax.random.fold_in(key_list[15], 71), 0),
        "final_gain": jnp.clip(1.0 + 0.18 * jax.random.normal(key_list[11], (D,), jnp.float32), 0.1, 1.9),
        "value_weight": normal_values(key_list[12], (D,), D ** -0.5, 0.09375, (), jnp.float32),
        "lm_head": draw_lm_head(jax.random.fold_in(key_list[15], 71), 0),
        "sampled": place_ends(jax.random.randint(key_list[14], (BATCH,), 0, VOCAB), jax.random.fold_in(key_list[14], 1), 0, VOCAB - 1).astype(jnp.int32),
    }


epsilon = 1e-06

def head_outputs(queries, keys_new, values_new, out_gate, decay_logit, beta_logit, decay_rate, state, norm_gain):
    rows_here, heads_here = decay_logit.shape
    query_f = queries.astype(jnp.float32).reshape(rows_here, heads_here, -1)
    key_f = keys_new.astype(jnp.float32).reshape(rows_here, heads_here, -1)
    value_f = values_new.astype(jnp.float32).reshape(rows_here, heads_here, -1)
    gate_f = out_gate.astype(jnp.float32).reshape(rows_here, heads_here, -1)
    key_size = query_f.shape[2]
    query_n = query_f / jnp.sqrt(lax.optimization_barrier(jnp.sum(query_f * query_f, axis=2, keepdims=True)) + epsilon)
    query_n = query_n * key_size ** (-0.5)
    key_n = key_f / jnp.sqrt(lax.optimization_barrier(jnp.sum(key_f * key_f, axis=2, keepdims=True)) + epsilon)
    decay = jnp.exp(-decay_rate[None, :] * jax.nn.softplus(decay_logit))
    strength = jax.nn.sigmoid(beta_logit)
    state_query = jnp.einsum('bhk,bhkv->bhv', query_n, state, precision=lax.Precision.HIGHEST)
    state_key = jnp.einsum('bhk,bhkv->bhv', key_n, state, precision=lax.Precision.HIGHEST)
    intersection = lax.optimization_barrier(jnp.sum(query_n * key_n, axis=2, keepdims=True))
    written = value_f - decay[..., None] * state_key
    output = decay[..., None] * state_query + strength[..., None] * intersection * written
    normed = output / jnp.sqrt(lax.optimization_barrier(jnp.mean(output * output, axis=2, keepdims=True)) + epsilon)
    result = normed * norm_gain * jax.nn.silu(gate_f)
    return result.reshape(rows_here, -1).astype(jnp.bfloat16)

def reference(queries, keys_new, values_new, out_gate, decay_logit, beta_logit, decay_rate, state, norm_gain, out_proj, residual, final_gain, value_weight, lm_head, sampled):
    headout = head_outputs(queries, keys_new, values_new, out_gate, decay_logit, beta_logit, decay_rate, state, norm_gain)
    attn = jnp.dot(headout, out_proj, preferred_element_type=jnp.float32)
    hsum = residual.astype(jnp.float32) + attn
    rstd = 1.0 / jnp.sqrt(lax.optimization_barrier(jnp.mean(hsum * hsum, axis=1)) + epsilon)
    value = rstd * lax.optimization_barrier(jnp.sum(hsum * final_gain * value_weight, axis=1))
    normed = (hsum * rstd[:, None] * final_gain).astype(jnp.bfloat16)
    logits = jnp.dot(normed, lm_head, preferred_element_type=jnp.float32)
    top = lax.optimization_barrier(jnp.max(logits, axis=1))
    total = lax.optimization_barrier(jnp.sum(jnp.exp(logits - top[:, None]), axis=1))
    chosen = jnp.take_along_axis(logits, sampled.astype(jnp.int32)[:, None], axis=1)[:, 0]
    logprob = chosen - (top + jnp.log(total))
    return (logprob, value)
```

```python
import functools

import jax
import jax.numpy as jnp
from jax import lax
from jax.experimental import pallas as pl
from jax.experimental.pallas import tpu as pltpu
from jax.sharding import PartitionSpec as P

MESH = pl.DeviceIdType.MESH
epsilon = 1e-06
f32 = jnp.float32
bf16 = jnp.bfloat16


def kernel(
    n_h,
    n_b,
    q_hbm,
    k_hbm,
    v_hbm,
    g_hbm,
    dl_hbm,
    bl_hbm,
    dr_hbm,
    state_hbm,
    ng_hbm,
    proj_hbm,
    res_hbm,
    fg_hbm,
    vw_hbm,
    lm_hbm,
    sampled_hbm,
    logprob_ref,
    value_ref,
    q_v,
    k_v,
    v_v,
    g_v,
    dl_v,
    bl_v,
    dr_v,
    st_v,
    ng_v,
    wp_v,
    res_v,
    fg_v,
    vw_v,
    lm_v,
    sampled_v,
    ho_v,
    part_v,
    rs_v,
    ssend_v,
    stat_v,
    gx_v,
    fx_v,
    small_sem,
    st_sem,
    wp_sem,
    rs_send,
    rs_recv,
    stat_send,
    stat_recv,
    g_send,
    g_recv,
    f_send,
    f_recv,
):
    n_all = n_h * n_b
    my_h = lax.axis_index("heads")
    my_b = lax.axis_index("batch")
    me = my_h * n_b + my_b
    my_y, my_c = my_h // 2, my_h % 2
    n_y = n_h // 2
    rows, width = q_v.shape
    heads_here = st_v.shape[1]
    size = st_v.shape[2]
    cols = res_v.shape[1]
    batch = sampled_v.shape[1]

    def peer(step):
        return ((my_y + 1 + step // 2) % n_y) * 2 + (my_c + step + 1) % 2

    early = [
        (q_hbm, q_v),
        (k_hbm, k_v),
        (v_hbm, v_v),
        (g_hbm, g_v),
        (dl_hbm, dl_v),
        (bl_hbm, bl_v),
        (dr_hbm, dr_v),
        (ng_hbm, ng_v),
    ]
    own_cols = pl.ds(pl.multiple_of(my_h * cols, cols), cols)
    late = [
        (res_hbm.at[:, own_cols], res_v),
        (fg_hbm.at[:, own_cols], fg_v),
        (vw_hbm.at[:, own_cols], vw_v),
        (lm_hbm, lm_v),
        (sampled_hbm, sampled_v),
    ]
    loads = [
        pltpu.make_async_copy(src, dst, small_sem.at[i])
        for i, (src, dst) in enumerate(early + late)
    ]
    n_early = len(early)
    for copy in loads[:n_early]:
        copy.start()
    st_loads = [
        pltpu.make_async_copy(state_hbm.at[:, h], st_v.at[:, h], st_sem.at[h])
        for h in range(heads_here)
    ]
    for copy in st_loads:
        copy.start()
    wp_loads = []
    for s in range(n_h):
        at = pl.ds(pl.multiple_of(peer(s) * cols, cols), cols)
        wp_loads.append(pltpu.make_async_copy(proj_hbm.at[:, at], wp_v.at[s], wp_sem.at[s]))
    for copy in wp_loads:
        copy.start()
    for copy in loads[n_early:]:
        copy.start()

    barrier = pltpu.get_barrier_semaphore()

    def greet(o, carry):
        other = (me + o) % n_all
        pl.semaphore_signal(
            barrier, inc=1, device_id=(other // n_b, other % n_b), device_id_type=MESH
        )
        return carry

    lax.fori_loop(1, n_all, greet, 0)

    for copy in loads[:n_early]:
        copy.wait()

    x = dl_v[...]
    softplus = jnp.maximum(x, 0.0) + jnp.log1p(jnp.exp(-jnp.abs(x)))
    decay_all = jnp.exp(-dr_v[...] * softplus)
    strength_all = 1.0 / (1.0 + jnp.exp(-bl_v[...]))
    head_lane = lax.broadcasted_iota(jnp.int32, x.shape, 1)
    norm_gain = ng_v[...]

    def head(h, carry):
        pltpu.make_async_copy(state_hbm.at[:, h], st_v.at[:, h], st_sem.at[h]).wait()
        at = pl.ds(pl.multiple_of(h * size, size), size)
        q = q_v[:, at].astype(f32)
        k = k_v[:, at].astype(f32)
        v = v_v[:, at].astype(f32)
        g = g_v[:, at].astype(f32)
        qn = q / jnp.sqrt(jnp.sum(q * q, axis=1, keepdims=True) + epsilon) * size ** (-0.5)
        kn = k / jnp.sqrt(jnp.sum(k * k, axis=1, keepdims=True) + epsilon)
        cross = jnp.sum(qn * kn, axis=1, keepdims=True)
        here = head_lane == h
        decay = jnp.sum(jnp.where(here, decay_all, 0.0), axis=1, keepdims=True)
        strength = jnp.sum(jnp.where(here, strength_all, 0.0), axis=1, keepdims=True)
        qt = qn.T
        kt = kn.T
        sq, sk = [], []
        for b in range(rows):
            s = st_v[b, h]
            sq.append(jnp.sum(qt[:, b : b + 1] * s, axis=0, keepdims=True))
            sk.append(jnp.sum(kt[:, b : b + 1] * s, axis=0, keepdims=True))
        sq = jnp.concatenate(sq, axis=0)
        sk = jnp.concatenate(sk, axis=0)
        o = decay * sq + strength * cross * (v - decay * sk)
        o = o / jnp.sqrt(jnp.mean(o * o, axis=1, keepdims=True) + epsilon)
        ho_v[:, at] = o * norm_gain * (g / (1.0 + jnp.exp(-g)))
        return carry

    lax.fori_loop(0, heads_here, head, 0)
    headout = ho_v[...].astype(bf16)

    rs_copies = []
    own = None
    for s in range(n_h):
        wp_loads[s].wait()
        part = jnp.dot(headout, wp_v[s], preferred_element_type=f32)
        if s == n_h - 1:
            own = part
            break
        part_v[s] = part
        if s == 0:
            pl.semaphore_wait(barrier, n_all - 1)
        copy = pltpu.make_async_remote_copy(
            src_ref=part_v.at[s],
            dst_ref=rs_v.at[s],
            send_sem=rs_send.at[s],
            recv_sem=rs_recv.at[s],
            device_id=(peer(s), my_b),
            device_id_type=MESH,
        )
        copy.start()
        rs_copies.append(copy)

    for copy in loads[n_early:]:
        copy.wait()
    hsum = res_v[...].astype(f32) + own
    for s in range(n_h - 1):
        rs_copies[s].wait_recv()
        hsum = hsum + rs_v[s]

    gain = fg_v[...]
    square = jnp.sum(hsum * hsum, axis=1, keepdims=True)
    weighed = jnp.sum(hsum * gain * vw_v[...], axis=1, keepdims=True)
    lane = lax.broadcasted_iota(jnp.int32, ssend_v.shape, 1)
    half = ssend_v.shape[1] // 2
    total = jnp.where(lane < half, square, weighed)
    ssend_v[...] = total
    stat_copies = []
    for s in range(n_h - 1):
        copy = pltpu.make_async_remote_copy(
            src_ref=ssend_v,
            dst_ref=stat_v.at[s],
            send_sem=stat_send.at[s],
            recv_sem=stat_recv.at[s],
            device_id=(peer(s), my_b),
            device_id_type=MESH,
        )
        copy.start()
        stat_copies.append(copy)
    for s in range(n_h - 1):
        stat_copies[s].wait_recv()
        total = total + stat_v[s]
    width_all = cols * n_h
    rstd = 1.0 / jnp.sqrt(total[:, :1] / width_all + epsilon)
    gx_v[me] = (hsum * rstd * gain).astype(bf16)

    def spread(o, carry):
        other = (me + o) % n_all
        other_h = other // n_b
        pltpu.make_async_remote_copy(
            src_ref=gx_v.at[me],
            dst_ref=gx_v.at[me],
            send_sem=g_send,
            recv_sem=g_recv.at[(my_h - other_h + n_h) % n_h],
            device_id=(other_h, other % n_b),
            device_id_type=MESH,
        ).start()
        return carry

    lax.fori_loop(1, n_all, spread, 0)

    value = rstd * total[:, half : half + 1]
    row_of = lax.broadcasted_iota(jnp.int32, ssend_v.shape, 0)
    value_ref[...] = jnp.sum(jnp.where(row_of == lane, value, 0.0), axis=0, keepdims=True)[:, :rows]

    logits = None
    for r in range(n_h):
        other_h = (my_h + r) % n_h
        arrived = gx_v.at[pl.ds(0, n_b if r else n_b - 1)]
        pltpu.make_async_copy(arrived, arrived, g_recv.at[r]).wait()
        block = jnp.concatenate(
            [gx_v[other_h * n_b + b].astype(f32) for b in range(n_b)], axis=0
        ).astype(bf16)
        at = pl.ds(pl.multiple_of(other_h * cols, cols), cols)
        term = jnp.dot(block, lm_v[at, :], preferred_element_type=f32)
        logits = term if logits is None else logits + term

    logits = logits.T
    vocab_own = lm_v.shape[1]
    ids = lax.broadcasted_iota(jnp.int32, logits.shape, 0) + me * vocab_own
    chosen = jnp.sum(jnp.where(ids == sampled_v[...], logits, 0.0), axis=0, keepdims=True)
    top = jnp.max(logits, axis=0, keepdims=True)
    mass = jnp.sum(jnp.exp(logits - top), axis=0, keepdims=True)
    fx_v[me, 0:1, :batch] = top + jnp.log(mass)
    fx_v[me, 1:2, :batch] = chosen

    def tell(o, carry):
        other = (me + o) % n_all
        pltpu.make_async_remote_copy(
            src_ref=fx_v.at[me],
            dst_ref=fx_v.at[me],
            send_sem=f_send,
            recv_sem=f_recv,
            device_id=(other // n_b, other % n_b),
            device_id_type=MESH,
        ).start()
        return carry

    lax.fori_loop(1, n_all, tell, 0)
    arrived = fx_v.at[pl.ds(0, n_all - 1)]
    pltpu.make_async_copy(arrived, arrived, f_recv).wait()

    both = fx_v[...]
    lse = both[:, 0, :]
    picked = jnp.sum(both[:, 1, :], axis=0, keepdims=True)
    best = jnp.max(lse, axis=0, keepdims=True)
    every = picked - (best + jnp.log(jnp.sum(jnp.exp(lse - best), axis=0, keepdims=True)))
    lanes = every.shape[1]
    pick = lax.broadcasted_iota(jnp.int32, (rows, lanes), 1) == (
        lax.broadcasted_iota(jnp.int32, (rows, lanes), 0) + my_b * rows
    )
    column = jnp.sum(jnp.where(pick, every, 0.0), axis=1, keepdims=True)
    logprob_ref[...] = jnp.sum(jnp.where(row_of == lane, column, 0.0), axis=0, keepdims=True)[
        :, :rows
    ]

    for s in range(n_h - 1):
        rs_copies[s].wait_send()
        stat_copies[s].wait_send()
    sent = gx_v.at[pl.ds(0, n_all - 1)]
    pltpu.make_async_copy(sent, sent, g_send).wait()
    sent = fx_v.at[pl.ds(0, n_all - 1)]
    pltpu.make_async_copy(sent, sent, f_send).wait()


def solution(mesh):
    n_h, n_b = mesh.shape["heads"], mesh.shape["batch"]

    def per_device(
        queries,
        keys_new,
        values_new,
        out_gate,
        decay_logit,
        beta_logit,
        decay_rate,
        state,
        norm_gain,
        out_proj,
        residual,
        final_gain,
        value_weight,
        lm_head,
        sampled,
    ):
        rows, width = queries.shape
        cols = out_proj.shape[1] // n_h
        n_all = n_h * n_b
        batch = sampled.shape[0]
        heads_here = state.shape[1]
        padded = max(batch, 128)
        like = lambda a: pltpu.VMEM(a.shape, a.dtype)
        decay_rate, norm_gain, final_gain, value_weight, sampled = (
            a.reshape(1, -1) for a in (decay_rate, norm_gain, final_gain, value_weight, sampled)
        )
        scratch = [
            like(queries),
            like(keys_new),
            like(values_new),
            like(out_gate),
            like(decay_logit),
            like(beta_logit),
            like(decay_rate),
            like(state),
            like(norm_gain),
            pltpu.VMEM((n_h, width, cols), bf16),
            pltpu.VMEM((rows, cols), bf16),
            pltpu.VMEM((1, cols), f32),
            pltpu.VMEM((1, cols), f32),
            like(lm_head),
            like(sampled),
            pltpu.VMEM((rows, width), f32),
            pltpu.VMEM((n_h - 1, rows, cols), f32),
            pltpu.VMEM((n_h - 1, rows, cols), f32),
            pltpu.VMEM((rows, 128), f32),
            pltpu.VMEM((n_h - 1, rows, 128), f32),
            pltpu.VMEM((n_all, rows, cols), bf16),
            pltpu.VMEM((n_all, 2, padded), f32),
            pltpu.SemaphoreType.DMA((13,)),
            pltpu.SemaphoreType.DMA((heads_here,)),
            pltpu.SemaphoreType.DMA((n_h,)),
            pltpu.SemaphoreType.DMA((n_h - 1,)),
            pltpu.SemaphoreType.DMA((n_h - 1,)),
            pltpu.SemaphoreType.DMA((n_h - 1,)),
            pltpu.SemaphoreType.DMA((n_h - 1,)),
            pltpu.SemaphoreType.DMA,
            pltpu.SemaphoreType.DMA((n_h,)),
            pltpu.SemaphoreType.DMA,
            pltpu.SemaphoreType.DMA,
        ]
        logprob, value = pl.pallas_call(
            functools.partial(kernel, n_h, n_b),
            out_shape=(
                jax.ShapeDtypeStruct((1, rows), f32),
                jax.ShapeDtypeStruct((1, rows), f32),
            ),
            in_specs=[pl.BlockSpec(memory_space=pl.ANY)] * 15,
            out_specs=(
                pl.BlockSpec(memory_space=pltpu.VMEM),
                pl.BlockSpec(memory_space=pltpu.VMEM),
            ),
            scratch_shapes=scratch,
            compiler_params=pltpu.CompilerParams(
                collective_id=0, has_side_effects=True, vmem_limit_bytes=48 * 1024 * 1024
            ),
        )(
            queries,
            keys_new,
            values_new,
            out_gate,
            decay_logit,
            beta_logit,
            decay_rate,
            state,
            norm_gain,
            out_proj,
            residual,
            final_gain,
            value_weight,
            lm_head,
            sampled,
        )
        return logprob.reshape(rows), value.reshape(rows)

    placed = (
        P("batch", "heads"),
        P("batch", "heads"),
        P("batch", "heads"),
        P("batch", "heads"),
        P("batch", "heads"),
        P("batch", "heads"),
        P("heads"),
        P("batch", "heads", None, None),
        P(),
        P("heads", None),
        P("batch", None),
        P(),
        P(),
        P(None, ("heads", "batch")),
        P(),
    )
    return jax.shard_map(
        per_device, mesh=mesh, in_specs=placed, out_specs=(P("batch"), P("batch")), check_vma=False
    )
```

```python
import functools

import jax
import jax.numpy as jnp
from jax import lax
from jax.experimental import pallas as pl
from jax.experimental.pallas import tpu as pltpu
from jax.sharding import PartitionSpec as P

MESH = pl.DeviceIdType.MESH
epsilon = 1e-06
f32 = jnp.float32
bf16 = jnp.bfloat16


def kernel(
    n_h,
    n_b,
    q_hbm,
    k_hbm,
    v_hbm,
    g_hbm,
    dl_hbm,
    bl_hbm,
    dr_hbm,
    state_hbm,
    ng_hbm,
    proj_hbm,
    res_hbm,
    fg_hbm,
    vw_hbm,
    lm_hbm,
    sampled_hbm,
    logprob_ref,
    value_ref,
    q_v,
    k_v,
    v_v,
    g_v,
    dl_v,
    bl_v,
    dr_v,
    st_v,
    ng_v,
    wp_v,
    res_v,
    fg_v,
    vw_v,
    lm_v,
    sampled_v,
    ho_v,
    part_v,
    rs_v,
    ssend_v,
    stat_v,
    gx_v,
    fx_v,
    small_sem,
    st_sem,
    wp_sem,
    rs_send,
    rs_recv,
    stat_send,
    stat_recv,
    g_send,
    z_recv,
    g_recv,
    p_recv,
    f_send,
    f_recv,
):
    n_all = n_h * n_b
    my_h = lax.axis_index("heads")
    my_b = lax.axis_index("batch")
    me = my_h * n_b + my_b
    my_y, my_c = my_h // 2, my_h % 2
    n_y = n_h // 2
    my_z, my_x = my_b // 2, my_b % 2
    n_z = n_b // 2
    n_p = n_y * 2
    upper = my_z * 2 // n_z
    rows, width = q_v.shape
    heads_here = st_v.shape[1]
    size = st_v.shape[2]
    cols = res_v.shape[1]
    batch = sampled_v.shape[1]

    def peer(step):
        return ((my_y + 1 + step // 2) % n_y) * 2 + (my_c + step + 1) % 2

    early = [
        (q_hbm, q_v),
        (k_hbm, k_v),
        (v_hbm, v_v),
        (g_hbm, g_v),
        (dl_hbm, dl_v),
        (bl_hbm, bl_v),
        (dr_hbm, dr_v),
        (ng_hbm, ng_v),
    ]
    own_cols = pl.ds(pl.multiple_of(my_h * cols, cols), cols)
    late = [
        (res_hbm.at[:, own_cols], res_v),
        (fg_hbm.at[:, own_cols], fg_v),
        (vw_hbm.at[:, own_cols], vw_v),
        (lm_hbm, lm_v),
        (sampled_hbm, sampled_v),
    ]
    loads = [
        pltpu.make_async_copy(src, dst, small_sem.at[i])
        for i, (src, dst) in enumerate(early + late)
    ]
    n_early = len(early)
    for copy in loads[:n_early]:
        copy.start()
    st_loads = [
        pltpu.make_async_copy(state_hbm.at[:, h], st_v.at[:, h], st_sem.at[h])
        for h in range(heads_here)
    ]
    for copy in st_loads:
        copy.start()
    wp_loads = []
    for s in range(n_h):
        at = pl.ds(pl.multiple_of(peer(s) * cols, cols), cols)
        wp_loads.append(pltpu.make_async_copy(proj_hbm.at[:, at], wp_v.at[s], wp_sem.at[s]))
    for copy in wp_loads:
        copy.start()
    for copy in loads[n_early:]:
        copy.start()

    barrier = pltpu.get_barrier_semaphore()

    def greet(o, carry):
        other = (me + o) % n_all
        pl.semaphore_signal(
            barrier, inc=1, device_id=(other // n_b, other % n_b), device_id_type=MESH
        )
        return carry

    lax.fori_loop(1, n_all, greet, 0)

    for copy in loads[:n_early]:
        copy.wait()

    x = dl_v[...]
    softplus = jnp.maximum(x, 0.0) + jnp.log1p(jnp.exp(-jnp.abs(x)))
    decay_all = jnp.exp(-dr_v[...] * softplus)
    strength_all = 1.0 / (1.0 + jnp.exp(-bl_v[...]))
    head_lane = lax.broadcasted_iota(jnp.int32, x.shape, 1)
    norm_gain = ng_v[...]

    def head(h, carry):
        pltpu.make_async_copy(state_hbm.at[:, h], st_v.at[:, h], st_sem.at[h]).wait()
        at = pl.ds(pl.multiple_of(h * size, size), size)
        q = q_v[:, at].astype(f32)
        k = k_v[:, at].astype(f32)
        v = v_v[:, at].astype(f32)
        g = g_v[:, at].astype(f32)
        qn = q / jnp.sqrt(jnp.sum(q * q, axis=1, keepdims=True) + epsilon) * size ** (-0.5)
        kn = k / jnp.sqrt(jnp.sum(k * k, axis=1, keepdims=True) + epsilon)
        cross = jnp.sum(qn * kn, axis=1, keepdims=True)
        here = head_lane == h
        decay = jnp.sum(jnp.where(here, decay_all, 0.0), axis=1, keepdims=True)
        strength = jnp.sum(jnp.where(here, strength_all, 0.0), axis=1, keepdims=True)
        qt = qn.T
        kt = kn.T
        sq, sk = [], []
        for b in range(rows):
            s = st_v[b, h]
            sq.append(jnp.sum(qt[:, b : b + 1] * s, axis=0, keepdims=True))
            sk.append(jnp.sum(kt[:, b : b + 1] * s, axis=0, keepdims=True))
        sq = jnp.concatenate(sq, axis=0)
        sk = jnp.concatenate(sk, axis=0)
        o = decay * sq + strength * cross * (v - decay * sk)
        o = o / jnp.sqrt(jnp.mean(o * o, axis=1, keepdims=True) + epsilon)
        ho_v[:, at] = o * norm_gain * (g / (1.0 + jnp.exp(-g)))
        return carry

    lax.fori_loop(0, heads_here, head, 0)
    headout = ho_v[...].astype(bf16)

    rs_copies = []
    own = None
    for s in range(n_h):
        wp_loads[s].wait()
        part = jnp.dot(headout, wp_v[s], preferred_element_type=f32)
        if s == n_h - 1:
            own = part
            break
        part_v[s] = part
        if s == 0:
            pl.semaphore_wait(barrier, n_all - 1)
        copy = pltpu.make_async_remote_copy(
            src_ref=part_v.at[s],
            dst_ref=rs_v.at[s],
            send_sem=rs_send.at[s],
            recv_sem=rs_recv.at[s],
            device_id=(peer(s), my_b),
            device_id_type=MESH,
        )
        copy.start()
        rs_copies.append(copy)

    for copy in loads[n_early:]:
        copy.wait()
    hsum = res_v[...].astype(f32) + own
    for s in range(n_h - 1):
        rs_copies[s].wait_recv()
        hsum = hsum + rs_v[s]

    gain = fg_v[...]
    square = jnp.sum(hsum * hsum, axis=1, keepdims=True)
    weighed = jnp.sum(hsum * gain * vw_v[...], axis=1, keepdims=True)
    lane = lax.broadcasted_iota(jnp.int32, ssend_v.shape, 1)
    half = ssend_v.shape[1] // 2
    total = jnp.where(lane < half, square, weighed)
    ssend_v[...] = total
    stat_copies = []
    for s in range(n_h - 1):
        copy = pltpu.make_async_remote_copy(
            src_ref=ssend_v,
            dst_ref=stat_v.at[s],
            send_sem=stat_send.at[s],
            recv_sem=stat_recv.at[s],
            device_id=(peer(s), my_b),
            device_id_type=MESH,
        )
        copy.start()
        stat_copies.append(copy)
    for s in range(n_h - 1):
        stat_copies[s].wait_recv()
        total = total + stat_v[s]
    width_all = cols * n_h
    rstd = 1.0 / jnp.sqrt(total[:, :1] / width_all + epsilon)
    gx_v[me] = (hsum * rstd * gain).astype(bf16)

    def forward(slot, other_h, other_b, sem):
        pltpu.make_async_remote_copy(
            src_ref=gx_v.at[slot],
            dst_ref=gx_v.at[slot],
            send_sem=g_send,
            recv_sem=sem,
            device_id=(other_h, other_b),
            device_id_type=MESH,
        ).start()

    def to_partner(slot):
        forward(slot, my_y * 2 + 1 - my_c, my_b, p_recv)

    def to_plane(slot, z):
        for o in reversed(range(1, n_p)):
            other_h = ((my_y + o // 2) % n_y) * 2 + my_c
            forward(slot, other_h, my_z * 2 + (my_x + o) % 2, g_recv.at[o - 1, z])

    def line(i):
        base = my_z + upper * (n_z - 1 - 2 * my_z)
        k = i + (i + n_z - base) // n_z
        return k + upper * (n_z - 1 - 2 * k)

    for i in reversed(range(n_z - 1)):
        forward(me, my_h, line(i) * 2 + my_x, z_recv.at[my_z])
    to_plane(me, my_z)
    to_partner(me)

    value = rstd * total[:, half : half + 1]
    row_of = lax.broadcasted_iota(jnp.int32, ssend_v.shape, 0)
    value_ref[...] = jnp.sum(jnp.where(row_of == lane, value, 0.0), axis=0, keepdims=True)[:, :rows]

    def slab_wait(sem, count):
        slabs = gx_v.at[pl.ds(0, count)]
        pltpu.make_async_copy(slabs, slabs, sem).wait()

    for i in range(n_z - 1):
        z = line(i)
        slab_wait(z_recv.at[z], 1)
        slot = my_h * n_b + z * 2 + my_x
        to_plane(slot, z)
        to_partner(slot)

    for i in range(n_z):
        z = line(i - 1) if i else my_z
        for o in range(1, n_p):
            slab_wait(g_recv.at[o - 1, z], 1)
            from_h = ((my_y - o // 2 + n_y) % n_y) * 2 + my_c
            to_partner(from_h * n_b + z * 2 + (my_x + o) % 2)

    logits = None
    for r in range(n_h):
        if r == n_y:
            slab_wait(p_recv, n_all // 2)
        core = my_c if r < n_y else 1 - my_c
        other_h = ((my_y + r) % n_y) * 2 + core
        block = jnp.concatenate(
            [gx_v[other_h * n_b + b].astype(f32) for b in range(n_b)], axis=0
        ).astype(bf16)
        at = pl.ds(pl.multiple_of(other_h * cols, cols), cols)
        term = jnp.dot(block, lm_v[at, :], preferred_element_type=f32)
        logits = term if logits is None else logits + term

    logits = logits.T
    vocab_own = lm_v.shape[1]
    ids = lax.broadcasted_iota(jnp.int32, logits.shape, 0) + me * vocab_own
    chosen = jnp.sum(jnp.where(ids == sampled_v[...], logits, 0.0), axis=0, keepdims=True)
    top = jnp.max(logits, axis=0, keepdims=True)
    mass = jnp.sum(jnp.exp(logits - top), axis=0, keepdims=True)
    fx_v[me, 0:1, :batch] = top + jnp.log(mass)
    fx_v[me, 1:2, :batch] = chosen

    def tell(o, carry):
        other = (me + o) % n_all
        pltpu.make_async_remote_copy(
            src_ref=fx_v.at[me],
            dst_ref=fx_v.at[me],
            send_sem=f_send,
            recv_sem=f_recv,
            device_id=(other // n_b, other % n_b),
            device_id_type=MESH,
        ).start()
        return carry

    lax.fori_loop(1, n_all, tell, 0)
    arrived = fx_v.at[pl.ds(0, n_all - 1)]
    pltpu.make_async_copy(arrived, arrived, f_recv).wait()

    both = fx_v[...]
    lse = both[:, 0, :]
    picked = jnp.sum(both[:, 1, :], axis=0, keepdims=True)
    best = jnp.max(lse, axis=0, keepdims=True)
    every = picked - (best + jnp.log(jnp.sum(jnp.exp(lse - best), axis=0, keepdims=True)))
    lanes = every.shape[1]
    pick = lax.broadcasted_iota(jnp.int32, (rows, lanes), 1) == (
        lax.broadcasted_iota(jnp.int32, (rows, lanes), 0) + my_b * rows
    )
    column = jnp.sum(jnp.where(pick, every, 0.0), axis=1, keepdims=True)
    logprob_ref[...] = jnp.sum(jnp.where(row_of == lane, column, 0.0), axis=0, keepdims=True)[
        :, :rows
    ]

    for s in range(n_h - 1):
        rs_copies[s].wait_send()
        stat_copies[s].wait_send()
    sent = gx_v.at[pl.ds(0, n_all - 1)]
    pltpu.make_async_copy(sent, sent, g_send).wait()
    sent = fx_v.at[pl.ds(0, n_all - 1)]
    pltpu.make_async_copy(sent, sent, f_send).wait()


def solution(mesh):
    n_h, n_b = mesh.shape["heads"], mesh.shape["batch"]

    def per_device(
        queries,
        keys_new,
        values_new,
        out_gate,
        decay_logit,
        beta_logit,
        decay_rate,
        state,
        norm_gain,
        out_proj,
        residual,
        final_gain,
        value_weight,
        lm_head,
        sampled,
    ):
        rows, width = queries.shape
        cols = out_proj.shape[1] // n_h
        n_all = n_h * n_b
        batch = sampled.shape[0]
        heads_here = state.shape[1]
        padded = max(batch, 128)
        like = lambda a: pltpu.VMEM(a.shape, a.dtype)
        decay_rate, norm_gain, final_gain, value_weight, sampled = (
            a.reshape(1, -1) for a in (decay_rate, norm_gain, final_gain, value_weight, sampled)
        )
        scratch = [
            like(queries),
            like(keys_new),
            like(values_new),
            like(out_gate),
            like(decay_logit),
            like(beta_logit),
            like(decay_rate),
            like(state),
            like(norm_gain),
            pltpu.VMEM((n_h, width, cols), bf16),
            pltpu.VMEM((rows, cols), bf16),
            pltpu.VMEM((1, cols), f32),
            pltpu.VMEM((1, cols), f32),
            like(lm_head),
            like(sampled),
            pltpu.VMEM((rows, width), f32),
            pltpu.VMEM((n_h - 1, rows, cols), f32),
            pltpu.VMEM((n_h - 1, rows, cols), f32),
            pltpu.VMEM((rows, 128), f32),
            pltpu.VMEM((n_h - 1, rows, 128), f32),
            pltpu.VMEM((n_all, rows, cols), bf16),
            pltpu.VMEM((n_all, 2, padded), f32),
            pltpu.SemaphoreType.DMA((13,)),
            pltpu.SemaphoreType.DMA((heads_here,)),
            pltpu.SemaphoreType.DMA((n_h,)),
            pltpu.SemaphoreType.DMA((n_h - 1,)),
            pltpu.SemaphoreType.DMA((n_h - 1,)),
            pltpu.SemaphoreType.DMA((n_h - 1,)),
            pltpu.SemaphoreType.DMA((n_h - 1,)),
            pltpu.SemaphoreType.DMA,
            pltpu.SemaphoreType.DMA((n_b // 2,)),
            pltpu.SemaphoreType.DMA((n_h - 1, n_b // 2)),
            pltpu.SemaphoreType.DMA,
            pltpu.SemaphoreType.DMA,
            pltpu.SemaphoreType.DMA,
        ]
        logprob, value = pl.pallas_call(
            functools.partial(kernel, n_h, n_b),
            out_shape=(
                jax.ShapeDtypeStruct((1, rows), f32),
                jax.ShapeDtypeStruct((1, rows), f32),
            ),
            in_specs=[pl.BlockSpec(memory_space=pl.ANY)] * 15,
            out_specs=(
                pl.BlockSpec(memory_space=pltpu.VMEM),
                pl.BlockSpec(memory_space=pltpu.VMEM),
            ),
            scratch_shapes=scratch,
            compiler_params=pltpu.CompilerParams(
                collective_id=0, has_side_effects=True, vmem_limit_bytes=67043328
            ),
        )(
            queries,
            keys_new,
            values_new,
            out_gate,
            decay_logit,
            beta_logit,
            decay_rate,
            state,
            norm_gain,
            out_proj,
            residual,
            final_gain,
            value_weight,
            lm_head,
            sampled,
        )
        return logprob.reshape(rows), value.reshape(rows)

    placed = (
        P("batch", "heads"),
        P("batch", "heads"),
        P("batch", "heads"),
        P("batch", "heads"),
        P("batch", "heads"),
        P("batch", "heads"),
        P("heads"),
        P("batch", "heads", None, None),
        P(),
        P("heads", None),
        P("batch", None),
        P(),
        P(),
        P(None, ("heads", "batch")),
        P(),
    )
    return jax.shard_map(
        per_device, mesh=mesh, in_specs=placed, out_specs=(P("batch"), P("batch")), check_vma=False
    )
```

```python
import functools

import jax
import jax.numpy as jnp
from jax import lax
from jax.experimental import pallas as pl
from jax.experimental.pallas import tpu as pltpu
from jax.sharding import PartitionSpec as P

MESH = pl.DeviceIdType.MESH
epsilon = 1e-06
f32 = jnp.float32
bf16 = jnp.bfloat16


def kernel(
    n_h,
    n_b,
    q_hbm,
    k_hbm,
    v_hbm,
    g_hbm,
    dl_hbm,
    bl_hbm,
    dr_hbm,
    state_hbm,
    ng_hbm,
    proj_hbm,
    res_hbm,
    fg_hbm,
    vw_hbm,
    lm_hbm,
    sampled_hbm,
    logprob_ref,
    value_ref,
    q_v,
    k_v,
    v_v,
    g_v,
    dl_v,
    bl_v,
    dr_v,
    st_v,
    ng_v,
    wp_v,
    res_v,
    fg_v,
    vw_v,
    lm_v,
    sampled_v,
    ho_v,
    part_v,
    rs_v,
    ssend_v,
    stat_v,
    gx_v,
    fx_v,
    small_sem,
    st_sem,
    wp_sem,
    rs_send,
    rs_recv,
    stat_send,
    stat_recv,
    g_send,
    z_recv,
    g_recv,
    p_recv,
    f_send,
    f_recv,
):
    n_all = n_h * n_b
    my_h = lax.axis_index("heads")
    my_b = lax.axis_index("batch")
    me = my_h * n_b + my_b
    my_y, my_c = my_h // 2, my_h % 2
    n_y = n_h // 2
    my_z, my_x = my_b // 2, my_b % 2
    n_z = n_b // 2
    n_p = n_y * 2
    upper = my_z * 2 // n_z
    rows, width = q_v.shape
    heads_here = st_v.shape[1]
    size = st_v.shape[2]
    cols = res_v.shape[1]
    batch = sampled_v.shape[1]

    def peer(step):
        return ((my_y + 1 + step // 2) % n_y) * 2 + (my_c + step + 1) % 2

    early = [
        (q_hbm, q_v),
        (k_hbm, k_v),
        (v_hbm, v_v),
        (g_hbm, g_v),
        (dl_hbm, dl_v),
        (bl_hbm, bl_v),
        (dr_hbm, dr_v),
        (ng_hbm, ng_v),
    ]
    own_cols = pl.ds(pl.multiple_of(my_h * cols, cols), cols)
    late = [
        (res_hbm.at[:, own_cols], res_v),
        (fg_hbm.at[:, own_cols], fg_v),
        (vw_hbm.at[:, own_cols], vw_v),
        (lm_hbm, lm_v),
        (sampled_hbm, sampled_v),
    ]
    loads = [
        pltpu.make_async_copy(src, dst, small_sem.at[i])
        for i, (src, dst) in enumerate(early + late)
    ]
    n_early = len(early)
    for copy in loads[:n_early]:
        copy.start()
    st_loads = [
        pltpu.make_async_copy(state_hbm.at[:, h], st_v.at[:, h], st_sem.at[h])
        for h in range(heads_here)
    ]
    for copy in st_loads:
        copy.start()
    wp_loads = []
    for s in range(n_h):
        at = pl.ds(pl.multiple_of(peer(s) * cols, cols), cols)
        wp_loads.append(pltpu.make_async_copy(proj_hbm.at[:, at], wp_v.at[s], wp_sem.at[s]))
    for copy in wp_loads:
        copy.start()
    for copy in loads[n_early:]:
        copy.start()

    barrier = pltpu.get_barrier_semaphore()

    others = [
        ((my_h + dh) % n_h, (my_b + db) % n_b)
        for dh in reversed(range(n_h))
        for db in reversed(range(n_b))
        if dh or db
    ]
    for other in others:
        pl.semaphore_signal(barrier, inc=1, device_id=other, device_id_type=MESH)

    for copy in loads[:n_early]:
        copy.wait()

    x = dl_v[...]
    softplus = jnp.maximum(x, 0.0) + jnp.log1p(jnp.exp(-jnp.abs(x)))
    decay_all = jnp.exp(-dr_v[...] * softplus)
    strength_all = 1.0 / (1.0 + jnp.exp(-bl_v[...]))
    head_lane = lax.broadcasted_iota(jnp.int32, x.shape, 1)
    norm_gain = ng_v[...]

    def head(h, carry):
        pltpu.make_async_copy(state_hbm.at[:, h], st_v.at[:, h], st_sem.at[h]).wait()
        at = pl.ds(pl.multiple_of(h * size, size), size)
        q = q_v[:, at].astype(f32)
        k = k_v[:, at].astype(f32)
        v = v_v[:, at].astype(f32)
        g = g_v[:, at].astype(f32)
        qn = q / jnp.sqrt(jnp.sum(q * q, axis=1, keepdims=True) + epsilon) * size ** (-0.5)
        kn = k / jnp.sqrt(jnp.sum(k * k, axis=1, keepdims=True) + epsilon)
        cross = jnp.sum(qn * kn, axis=1, keepdims=True)
        here = head_lane == h
        decay = jnp.sum(jnp.where(here, decay_all, 0.0), axis=1, keepdims=True)
        strength = jnp.sum(jnp.where(here, strength_all, 0.0), axis=1, keepdims=True)
        qt = qn.T
        kt = kn.T
        sq, sk = [], []
        for b in range(rows):
            s = st_v[b, h]
            sq.append(jnp.sum(qt[:, b : b + 1] * s, axis=0, keepdims=True))
            sk.append(jnp.sum(kt[:, b : b + 1] * s, axis=0, keepdims=True))
        sq = jnp.concatenate(sq, axis=0)
        sk = jnp.concatenate(sk, axis=0)
        o = decay * sq + strength * cross * (v - decay * sk)
        o = o / jnp.sqrt(jnp.mean(o * o, axis=1, keepdims=True) + epsilon)
        ho_v[:, at] = o * norm_gain * (g / (1.0 + jnp.exp(-g)))
        return carry

    lax.fori_loop(0, heads_here, head, 0)
    headout = ho_v[...].astype(bf16)

    rs_copies = []
    own = None
    for s in range(n_h):
        wp_loads[s].wait()
        part = jnp.dot(headout, wp_v[s], preferred_element_type=f32)
        if s == n_h - 1:
            own = part
            break
        part_v[s] = part
        if s == 0:
            pl.semaphore_wait(barrier, n_all - 1)
        copy = pltpu.make_async_remote_copy(
            src_ref=part_v.at[s],
            dst_ref=rs_v.at[s],
            send_sem=rs_send.at[s],
            recv_sem=rs_recv.at[s],
            device_id=(peer(s), my_b),
            device_id_type=MESH,
        )
        copy.start()
        rs_copies.append(copy)

    for copy in loads[n_early:]:
        copy.wait()
    hsum = res_v[...].astype(f32) + own
    for s in range(n_h - 1):
        rs_copies[s].wait_recv()
        hsum = hsum + rs_v[s]

    gain = fg_v[...]
    square = jnp.sum(hsum * hsum, axis=1, keepdims=True)
    weighed = jnp.sum(hsum * gain * vw_v[...], axis=1, keepdims=True)
    lane = lax.broadcasted_iota(jnp.int32, ssend_v.shape, 1)
    half = ssend_v.shape[1] // 2
    total = jnp.where(lane < half, square, weighed)
    ssend_v[...] = total
    stat_copies = []
    for s in range(n_h - 1):
        copy = pltpu.make_async_remote_copy(
            src_ref=ssend_v,
            dst_ref=stat_v.at[s],
            send_sem=stat_send.at[s],
            recv_sem=stat_recv.at[s],
            device_id=(peer(s), my_b),
            device_id_type=MESH,
        )
        copy.start()
        stat_copies.append(copy)
    for s in range(n_h - 1):
        stat_copies[s].wait_recv()
        total = total + stat_v[s]
    width_all = cols * n_h
    rstd = 1.0 / jnp.sqrt(total[:, :1] / width_all + epsilon)
    gx_v[me] = (hsum * rstd * gain).astype(bf16)

    def forward(slot, other_h, other_b, sem):
        pltpu.make_async_remote_copy(
            src_ref=gx_v.at[slot],
            dst_ref=gx_v.at[slot],
            send_sem=g_send,
            recv_sem=sem,
            device_id=(other_h, other_b),
            device_id_type=MESH,
        ).start()

    def to_partner(slot):
        forward(slot, my_y * 2 + 1 - my_c, my_b, p_recv)

    def to_plane(slot, z):
        for o in reversed(range(1, n_p)):
            other_h = ((my_y + o // 2) % n_y) * 2 + my_c
            forward(slot, other_h, my_z * 2 + (my_x + o) % 2, g_recv.at[o - 1, z])

    def line(i):
        base = my_z + upper * (n_z - 1 - 2 * my_z)
        k = i + (i + n_z - base) // n_z
        return k + upper * (n_z - 1 - 2 * k)

    for i in reversed(range(n_z - 1)):
        forward(me, my_h, line(i) * 2 + my_x, z_recv.at[my_z])
    to_plane(me, my_z)
    to_partner(me)

    value = rstd * total[:, half : half + 1]
    row_of = lax.broadcasted_iota(jnp.int32, ssend_v.shape, 0)
    value_ref[...] = jnp.sum(jnp.where(row_of == lane, value, 0.0), axis=0, keepdims=True)[:, :rows]

    def slab_wait(sem, count):
        slabs = gx_v.at[pl.ds(0, count)]
        pltpu.make_async_copy(slabs, slabs, sem).wait()

    for i in range(n_z - 1):
        z = line(i)
        slab_wait(z_recv.at[z], 1)
        slot = my_h * n_b + z * 2 + my_x
        to_plane(slot, z)
        to_partner(slot)

    for i in range(n_z):
        z = line(i - 1) if i else my_z
        for o in range(1, n_p):
            slab_wait(g_recv.at[o - 1, z], 1)
            from_h = ((my_y - o // 2 + n_y) % n_y) * 2 + my_c
            to_partner(from_h * n_b + z * 2 + (my_x + o) % 2)

    logits = None
    for r in range(n_h):
        if r == n_y:
            slab_wait(p_recv, n_all // 2)
        core = my_c if r < n_y else 1 - my_c
        other_h = ((my_y + r) % n_y) * 2 + core
        block = jnp.concatenate(
            [gx_v[other_h * n_b + b].astype(f32) for b in range(n_b)], axis=0
        ).astype(bf16)
        at = pl.ds(pl.multiple_of(other_h * cols, cols), cols)
        term = jnp.dot(block, lm_v[at, :], preferred_element_type=f32)
        logits = term if logits is None else logits + term

    logits = logits.T
    vocab_own = lm_v.shape[1]
    ids = lax.broadcasted_iota(jnp.int32, logits.shape, 0) + me * vocab_own
    chosen = jnp.sum(jnp.where(ids == sampled_v[...], logits, 0.0), axis=0, keepdims=True)
    top = jnp.max(logits, axis=0, keepdims=True)
    mass = jnp.sum(jnp.exp(logits - top), axis=0, keepdims=True)
    fx_v[me, 0:1, :batch] = top + jnp.log(mass)
    fx_v[me, 1:2, :batch] = chosen

    for other in others:
        pltpu.make_async_remote_copy(
            src_ref=fx_v.at[me],
            dst_ref=fx_v.at[me],
            send_sem=f_send,
            recv_sem=f_recv,
            device_id=other,
            device_id_type=MESH,
        ).start()
    arrived = fx_v.at[pl.ds(0, n_all - 1)]
    pltpu.make_async_copy(arrived, arrived, f_recv).wait()

    both = fx_v[...]
    lse = both[:, 0, :]
    picked = jnp.sum(both[:, 1, :], axis=0, keepdims=True)
    best = jnp.max(lse, axis=0, keepdims=True)
    every = picked - (best + jnp.log(jnp.sum(jnp.exp(lse - best), axis=0, keepdims=True)))
    lanes = every.shape[1]
    pick = lax.broadcasted_iota(jnp.int32, (rows, lanes), 1) == (
        lax.broadcasted_iota(jnp.int32, (rows, lanes), 0) + my_b * rows
    )
    column = jnp.sum(jnp.where(pick, every, 0.0), axis=1, keepdims=True)
    logprob_ref[...] = jnp.sum(jnp.where(row_of == lane, column, 0.0), axis=0, keepdims=True)[
        :, :rows
    ]

    for s in range(n_h - 1):
        rs_copies[s].wait_send()
        stat_copies[s].wait_send()
    sent = gx_v.at[pl.ds(0, n_all - 1)]
    pltpu.make_async_copy(sent, sent, g_send).wait()
    sent = fx_v.at[pl.ds(0, n_all - 1)]
    pltpu.make_async_copy(sent, sent, f_send).wait()


def solution(mesh):
    n_h, n_b = mesh.shape["heads"], mesh.shape["batch"]

    def per_device(
        queries,
        keys_new,
        values_new,
        out_gate,
        decay_logit,
        beta_logit,
        decay_rate,
        state,
        norm_gain,
        out_proj,
        residual,
        final_gain,
        value_weight,
        lm_head,
        sampled,
    ):
        rows, width = queries.shape
        cols = out_proj.shape[1] // n_h
        n_all = n_h * n_b
        batch = sampled.shape[0]
        heads_here = state.shape[1]
        padded = max(batch, 128)
        like = lambda a: pltpu.VMEM(a.shape, a.dtype)
        decay_rate, norm_gain, final_gain, value_weight, sampled = (
            a.reshape(1, -1) for a in (decay_rate, norm_gain, final_gain, value_weight, sampled)
        )
        scratch = [
            like(queries),
            like(keys_new),
            like(values_new),
            like(out_gate),
            like(decay_logit),
            like(beta_logit),
            like(decay_rate),
            like(state),
            like(norm_gain),
            pltpu.VMEM((n_h, width, cols), bf16),
            pltpu.VMEM((rows, cols), bf16),
            pltpu.VMEM((1, cols), f32),
            pltpu.VMEM((1, cols), f32),
            like(lm_head),
            like(sampled),
            pltpu.VMEM((rows, width), f32),
            pltpu.VMEM((n_h - 1, rows, cols), f32),
            pltpu.VMEM((n_h - 1, rows, cols), f32),
            pltpu.VMEM((rows, 128), f32),
            pltpu.VMEM((n_h - 1, rows, 128), f32),
            pltpu.VMEM((n_all, rows, cols), bf16),
            pltpu.VMEM((n_all, 2, padded), f32),
            pltpu.SemaphoreType.DMA((13,)),
            pltpu.SemaphoreType.DMA((heads_here,)),
            pltpu.SemaphoreType.DMA((n_h,)),
            pltpu.SemaphoreType.DMA((n_h - 1,)),
            pltpu.SemaphoreType.DMA((n_h - 1,)),
            pltpu.SemaphoreType.DMA((n_h - 1,)),
            pltpu.SemaphoreType.DMA((n_h - 1,)),
            pltpu.SemaphoreType.DMA,
            pltpu.SemaphoreType.DMA((n_b // 2,)),
            pltpu.SemaphoreType.DMA((n_h - 1, n_b // 2)),
            pltpu.SemaphoreType.DMA,
            pltpu.SemaphoreType.DMA,
            pltpu.SemaphoreType.DMA,
        ]
        logprob, value = pl.pallas_call(
            functools.partial(kernel, n_h, n_b),
            out_shape=(
                jax.ShapeDtypeStruct((1, rows), f32),
                jax.ShapeDtypeStruct((1, rows), f32),
            ),
            in_specs=[pl.BlockSpec(memory_space=pl.ANY)] * 15,
            out_specs=(
                pl.BlockSpec(memory_space=pltpu.VMEM),
                pl.BlockSpec(memory_space=pltpu.VMEM),
            ),
            scratch_shapes=scratch,
            compiler_params=pltpu.CompilerParams(
                collective_id=0, has_side_effects=True, vmem_limit_bytes=67043328
            ),
        )(
            queries,
            keys_new,
            values_new,
            out_gate,
            decay_logit,
            beta_logit,
            decay_rate,
            state,
            norm_gain,
            out_proj,
            residual,
            final_gain,
            value_weight,
            lm_head,
            sampled,
        )
        return logprob.reshape(rows), value.reshape(rows)

    placed = (
        P("batch", "heads"),
        P("batch", "heads"),
        P("batch", "heads"),
        P("batch", "heads"),
        P("batch", "heads"),
        P("batch", "heads"),
        P("heads"),
        P("batch", "heads", None, None),
        P(),
        P("heads", None),
        P("batch", None),
        P(),
        P(),
        P(None, ("heads", "batch")),
        P(),
    )
    return jax.shard_map(
        per_device, mesh=mesh, in_specs=placed, out_specs=(P("batch"), P("batch")), check_vma=False
    )
```
